32 devices in a mesh: wrow: 4 (over y, core), wcol: 2 (over x), dom: 4 (over z).
Axes of the slice: x: 2, y: 2, z: 4, core: 2. Of those that a mesh axis runs over, the one named last changes fastest.
Arguments:
- positions: float32 [4, 2, 3, 8192], P('wrow', 'wcol', None, 'dom'), may hold values from -6 to 6
- velocities: float32 [4, 2, 3, 8192], P('wrow', 'wcol', None, 'dom'), may hold values from -6 to 6
- inv_mass: float32 [8192], P('dom'), may hold values from 0.5 to 2
- cv_weight: float32 [2, 3, 8192], P(None, None, 'dom'), may hold values from -0.125 to 0.125
- stiffness: float32 [2], replicated, may hold values from 1 to 4
- centers: float32 [4, 2, 2], P('wrow', 'wcol'), may hold values from -3 to 3
- block_order: int32 [8192], P('dom'), may hold values from 0 to 2047, as said below
- pair_count: int32 [4], P('dom'), may hold values from 16 to 64, as said below
- pair_own: int32 [4, 64], P('dom'), may hold values from 0 to 15, as said below
- pair_other: int32 [4, 64], P('dom'), may hold values from 0 to 47, as said below
- accept_row: int32 [4, 2], P('wrow', 'wcol'), may hold values from 0 to 1, as said below
- accept_col: int32 [4, 2], P('wrow', 'wcol'), may hold values from 0 to 1, as said below
Outputs:
- new_positions: float32 [4, 2, 3, 8192], P('wrow', 'wcol', None, 'dom')
- new_velocities: float32 [4, 2, 3, 8192], P('wrow', 'wcol', None, 'dom')
- new_forces: float32 [4, 2, 3, 8192], P('wrow', 'wcol', None, 'dom')
The draws below stay inside these ranges and needn't reach their ends.
Inputs may be any that keep to these rules, and one draw needn't show every extreme that they name: accept_row is equal for windows (2k, c) and (2k + 1, c). accept_col is equal for windows (r, 2k) and (r, 2k + 1). `block_order`: each slab's 2048 entries are a permutation of 0 to 2047. `pair_count`: some slab has exactly 64 live pairs. `pair_own`: entries past the slab's pair_count are 0. `pair_other`: slab 0 names no lower slab and the last slab no upper slab; entries past the slab's pair_count are 16.
All inputs are finite; a program needn't handle non-finite values.
Results may differ from the reference program's by a relative error of at most 0.0003.
Values sent between devices are 32-bit elements; how exact they have to be, the bound alone decides.
A program may use at most 64 MiB of HBM per device.

```python
import math
import jax
import jax.numpy as jnp
from jax import lax

ATOM_DEV = 2048
BLK = 128
STEPS = 3
NB = 16
PMAX = 64
ATOMS = 8192
NROW = 4
NCOL = 2


def counts_of(key):
    domains = ATOMS // ATOM_DEV
    base = jax.random.randint(jax.random.fold_in(key, 11), (domains,), PMAX // 4, PMAX + 1)
    chosen = jax.random.randint(jax.random.fold_in(key, 12), (), 0, domains)
    return jnp.where(jnp.arange(domains) == chosen, PMAX, base).astype(jnp.int32)


def live_slots(key):
    return jnp.arange(PMAX)[None, :] < counts_of(key)[:, None]


def draw_pair_count(key, part):
    return counts_of(key)


def draw_pair_own(key, part):
    domains = ATOMS // ATOM_DEV
    raw_blocks = jax.random.randint(jax.random.fold_in(key, 13), (domains, PMAX), 0, NB)
    return jnp.where(live_slots(key), raw_blocks, 0).astype(jnp.int32)


def draw_pair_other(key, part):
    domains = ATOMS // ATOM_DEV
    raw_blocks = jax.random.randint(jax.random.fold_in(key, 14), (domains, PMAX), 0, 3 * NB)
    slab_ids = jnp.arange(domains)[:, None]
    raw_blocks = jnp.where((slab_ids == 0) & (raw_blocks < NB), raw_blocks + NB, raw_blocks)
    raw_blocks = jnp.where((slab_ids == domains - 1) & (raw_blocks >= 2 * NB), raw_blocks - NB, raw_blocks)
    return jnp.where(live_slots(key), raw_blocks, NB).astype(jnp.int32)


def draw_block_order(key, part):
    domains = ATOMS // ATOM_DEV

    def one_slab(slab):
        return jax.random.permutation(jax.random.fold_in(key, 31 + slab), ATOM_DEV)
    return jax.vmap(one_slab)(jnp.arange(domains)).reshape(ATOMS).astype(jnp.int32)


def draw_accept_row(key, part):
    halves = jax.random.randint(jax.random.fold_in(key, 21), (NROW // 2, NCOL), 0, 2)
    halves = halves.at[0, 0].set(1).at[0, 1].set(0)
    return jnp.repeat(halves, 2, axis=0).astype(jnp.int32)


def draw_accept_col(key, part):
    halves = jax.random.randint(jax.random.fold_in(key, 22), (NROW, NCOL // 2), 0, 2)
    halves = halves.at[0, 0].set(1).at[1, 0].set(0)
    return jnp.repeat(halves, 2, axis=1).astype(jnp.int32)


def steps_of(stream_key, dims, cuts, smallest, largest):
    loudness = 1.0
    for axis_at, shards_of in cuts:
        heights = jax.random.uniform(jax.random.fold_in(jax.random.fold_in(stream_key, 6), axis_at), (shards_of,), jnp.float32, smallest / len(cuts), largest / len(cuts))
        loudness = loudness * jnp.repeat(jnp.exp(heights), dims[axis_at] // shards_of).reshape((-1,) + (1,) * (len(dims) - 1 - axis_at))
    return loudness


def scatter_about(key, extent, width, most, split=(), held_as=jnp.bfloat16):
    array = width * jax.random.normal(key, extent, jnp.float32)
    if split:
        array = array * steps_of(key, extent, split, -0.22, 0.18)
    return jnp.clip(array, -most, most).astype(held_as)


def setup_inputs(seed: int = 0) -> dict:
    seeds = jax.random.split(jax.random.key(seed), 13)
    return {
        "positions": scatter_about(seeds[0], (NROW, NCOL, 3, ATOMS), 1.0, 6.0, ((0, 4), (1, 2), (3, 4)), jnp.float32),
        "velocities": scatter_about(seeds[1], (NROW, NCOL, 3, ATOMS), 1.0, 6.0, ((0, 4), (1, 2), (3, 4)), jnp.float32),
        "inv_mass": jnp.clip(jnp.exp(math.log(2.0) - 1.3862944 * jax.random.uniform(seeds[2], (ATOMS,), jnp.float32) ** steps_of(seeds[2], (ATOMS,), ((0, 4),), -0.2, 0.2)), 0.5, 2.0),
        "cv_weight": scatter_about(seeds[3], (2, 3, ATOMS), ATOM_DEV ** -0.5, 0.125, ((2, 4),), jnp.float32),
        "stiffness": jnp.clip(jnp.exp(jax.random.uniform(seeds[4], (2,), jnp.float32, math.log(1.0), math.log(4.0))), 1.0, 4.0),
        "centers": jnp.clip(jax.random.uniform(seeds[5], (NROW, NCOL, 2), jnp.float32, -3.0, 3.0) * steps_of(seeds[5], (NROW, NCOL, 2), ((0, 4), (1, 2)), -0.4, 0.0), -3.0, 3.0),
        "block_order": draw_block_order(jax.random.fold_in(seeds[12], 71), 0),
        "pair_count": draw_pair_count(jax.random.fold_in(seeds[12], 71), 0),
        "pair_own": draw_pair_own(jax.random.fold_in(seeds[12], 71), 0),
        "pair_other": draw_pair_other(jax.random.fold_in(seeds[12], 71), 0),
        "accept_row": draw_accept_row(jax.random.fold_in(seeds[12], 71), 0),
        "accept_col": draw_accept_col(jax.random.fold_in(seeds[12], 71), 0),
    }


PAIR_EPS = 0.015625
DT = 0.1


def pair_tile(own_tile, other_tile):
    offsets = own_tile[:, :, None] - other_tile[:, None, :]
    squared = jnp.sum(offsets * offsets, axis=0)
    weight_tile = PAIR_EPS * jnp.exp(-0.5 * squared)
    return own_tile * jnp.sum(weight_tile, axis=1)[None, :] - jnp.dot(other_tile, weight_tile.T, precision=lax.Precision.HIGHEST)


def domain_forces(nearby, pair_total, own_blocks, other_blocks):
    blocks_dev = ATOM_DEV // BLK

    def add_tile(forces_acc, index):
        own_index = own_blocks[index]
        other_index = other_blocks[index]
        own_tile = lax.dynamic_slice(nearby, (jnp.int32(0), ((blocks_dev + own_index) * BLK).astype(jnp.int32)), (3, BLK))
        other_tile = lax.dynamic_slice(nearby, (jnp.int32(0), (other_index * BLK).astype(jnp.int32)), (3, BLK))
        live = (index < pair_total).astype(forces_acc.dtype)
        offset = (own_index * BLK).astype(jnp.int32)
        older = lax.dynamic_slice(forces_acc, (jnp.int32(0), offset), (3, BLK))
        forces_acc = lax.dynamic_update_slice(forces_acc, older + live * pair_tile(own_tile, other_tile), (jnp.int32(0), offset))
        return forces_acc, None

    forces_acc, _ = lax.scan(add_tile, jnp.zeros((3, ATOM_DEV), jnp.float32), jnp.arange(PMAX, dtype=jnp.int32))
    return forces_acc


def window_pair(coords, pair_count, pair_own, pair_other):
    domains = ATOMS // ATOM_DEV
    slab_rows = coords.reshape(3, domains, ATOM_DEV)
    zeros_slab = jnp.zeros((3, 1, ATOM_DEV), coords.dtype)
    padded = jnp.concatenate([zeros_slab, slab_rows, zeros_slab], axis=1)
    nearby = jnp.stack([padded[:, slab:slab + 3].reshape(3, 3 * ATOM_DEV) for slab in range(domains)])
    forces_all = jax.vmap(domain_forces)(nearby, pair_count, pair_own, pair_other)
    return jnp.transpose(forces_all, (1, 0, 2)).reshape(3, ATOMS)


def total_force(coords, weights, stiffness, centre_rows, pair_count, pair_own, pair_other):
    pair = jax.vmap(window_pair, in_axes=(0, None, None, None))(coords, pair_count, pair_own, pair_other)
    collective = jnp.sum(weights[None] * coords[:, None], axis=(2, 3))
    pull = stiffness[None, :] * (collective - centre_rows)
    return pair - jnp.sum(pull[:, :, None, None] * weights[None], axis=1)


def partner_select(state, flags, axis):
    count_axis = state.shape[axis]
    swapped = jnp.take(state, jnp.arange(count_axis, dtype=jnp.int32) ^ 1, axis=axis)
    return jnp.where((flags == 1)[:, :, None, None], swapped, state)


def reference(positions, velocities, inv_mass, cv_weight, stiffness, centers, block_order, pair_count, pair_own, pair_other, accept_row, accept_col):
    domains = ATOMS // ATOM_DEV
    windows = NROW * NCOL
    global_order = (block_order.reshape(domains, ATOM_DEV) + (jnp.arange(domains, dtype=jnp.int32) * ATOM_DEV)[:, None]).reshape(ATOMS).astype(jnp.int32)
    inverse = jnp.zeros((ATOMS,), jnp.int32).at[global_order].set(jnp.arange(ATOMS, dtype=jnp.int32))
    coords = positions.reshape(windows, 3, ATOMS)[:, :, global_order]
    speeds = velocities.reshape(windows, 3, ATOMS)[:, :, global_order]
    inverse_mass = inv_mass[global_order]
    weights = cv_weight[:, :, global_order]
    centre_rows = centers.reshape(windows, 2)
    forces_now = total_force(coords, weights, stiffness, centre_rows, pair_count, pair_own, pair_other)
    for _ in range(STEPS):
        speeds = speeds + (0.5 * DT) * inverse_mass * forces_now
        coords = coords + DT * speeds
        forces_now = total_force(coords, weights, stiffness, centre_rows, pair_count, pair_own, pair_other)
        speeds = speeds + (0.5 * DT) * inverse_mass * forces_now
    results = []
    for state in (coords, speeds, forces_now):
        state = state[:, :, inverse].reshape(NROW, NCOL, 3, ATOMS)
        state = partner_select(state, accept_row, 0)
        state = partner_select(state, accept_col, 1)
        results.append(state)
    return (results[0], results[1], results[2])
```

```python
import functools
import math

import jax
import jax.numpy as jnp
from jax import lax
from jax.experimental import pallas as pl
from jax.experimental.pallas import tpu as pltpu
from jax.sharding import PartitionSpec as P

BLK = 128
STEPS = 3
PAIR_EPS = 0.015625
DT = 0.1
SCALE = math.sqrt(0.5 * math.log2(math.e))
MESH = pl.DeviceIdType.MESH
F32 = jnp.float32
BF16 = jnp.bfloat16


def split3(value):
    high = value.astype(BF16)
    rest = value - high.astype(F32)
    middle = rest.astype(BF16)
    low = (rest - middle.astype(F32)).astype(BF16)
    return high, middle, low


def stacked_split(value):
    return jnp.concatenate(split3(value), axis=0)


def unsplit(value, rows):
    return value[0:rows] + (value[rows : 2 * rows] + value[2 * rows : 3 * rows])


def kernel(
    sizes,
    pos, vel, mass, cvw, order, own_row, own_s, other_s, count_s, stiff_s, centers_s, arow_s, acol_s,
    out_x, out_v, out_f,
    onehot, high_block, raw, raw_w, got_x, got_v, got_aux, aux, parts, tiles, xs, vs, fs, ms, ws,
    sx_send, sx_recv, sv_send, sv_recv, sa_send, sa_recv, halo_send, halo_recv, part_send, part_recv, *nears,
):
    doms, nb, slots = sizes
    row = lax.axis_index("wrow")
    col = lax.axis_index("wcol")
    me = lax.axis_index("dom")
    row_to = row + 1 - 2 * lax.rem(row, 2)
    col_to = col + 1 - 2 * lax.rem(col, 2)
    partners = [(row_to, col, me), (row, col_to, me), (row_to, col_to, me)]
    others = [(row, col, lax.rem(me + off, doms)) for off in range(1, doms)]

    lines = lax.broadcasted_iota(jnp.int32, (8, BLK), 0)
    aux[...] = jnp.where(
        lines == 0,
        centers_s[0, 0],
        jnp.where(lines == 1, centers_s[0, 1], arow_s[0, 0].astype(F32)),
    )
    for held in nears:
        held[...] = jnp.zeros(held.shape, F32)
    barrier = pltpu.get_barrier_semaphore()
    for target in partners + others:
        pl.semaphore_signal(barrier, inc=1, device_id=target, device_id_type=MESH)
    pl.semaphore_wait(barrier, len(partners) + len(others))

    def exchange(source, target, sends, recvs):
        copies = []
        for at, partner in enumerate(partners):
            copy = pltpu.make_async_remote_copy(
                src_ref=source,
                dst_ref=target.at[at],
                send_sem=sends.at[at],
                recv_sem=recvs.at[at],
                device_id=partner,
                device_id_type=MESH,
            )
            copy.start()
            copies.append(copy)
        return copies

    aux_copies = exchange(aux, got_aux, sa_send, sa_recv)
    x_copies = exchange(pos, got_x, sx_send, sx_recv)
    v_copies = exchange(vel, got_v, sv_send, sv_recv)

    jl = lax.broadcasted_iota(jnp.int32, (BLK, BLK), 0)
    listed = order[...]
    low = lax.rem(listed, BLK)
    high_block[...] = lax.div(listed, BLK)
    for b in range(nb):
        onehot[:, b * BLK : (b + 1) * BLK] = jnp.where(low[b : b + 1, :] == jl, 1.0, 0.0).astype(BF16)
    jb_lines = lax.broadcasted_iota(jnp.int32, (nb, BLK), 0)

    def permuted(source, comps, store):
        split = stacked_split(source)

        def body(b, carry):
            at = pl.ds(pl.multiple_of(b * BLK, BLK), BLK)
            picked = jnp.dot(split, onehot[:, at], preferred_element_type=F32)
            picked = unsplit(picked, comps * nb)
            mask = high_block[pl.ds(b, 1), :] == jb_lines
            for k in range(comps):
                line = jnp.sum(jnp.where(mask, picked[k * nb : (k + 1) * nb], 0.0), axis=0, keepdims=True)
                store(k, b, line)
            return carry

        lax.fori_loop(0, nb, body, 0)

    def unpermuted(source_ref):
        def body(b, total):
            at = pl.ds(pl.multiple_of(b * BLK, BLK), BLK)
            mask = high_block[pl.ds(b, 1), :] == jb_lines
            spread = jnp.concatenate(
                [jnp.where(mask, source_ref[k, pl.ds(b, 1), :], 0.0) for k in range(3)], axis=0
            )
            return total + lax.dot_general(
                stacked_split(spread), onehot[:, at], (((1,), (1,)), ((), ())), preferred_element_type=F32
            )

        total = lax.fori_loop(0, nb, body, jnp.zeros((9 * nb, BLK), F32))
        return unsplit(total, 3 * nb).reshape(3, nb, BLK)

    for b in range(nb):
        at = slice(b * BLK, (b + 1) * BLK)
        for k in range(2):
            for c in range(3):
                raw_w[(3 * k + c) * nb + b : (3 * k + c) * nb + b + 1, :] = cvw[k, c : c + 1, at]
    raw_w[6 * nb : 7 * nb, :] = mass[...]

    def store_w(k, b, line):
        if k < 6:
            ws[k // 3, k % 3, pl.ds(b, 1), :] = line
        else:
            ms[pl.ds(b, 1), :] = line

    permuted(raw_w[...], 7, store_w)

    own_mask = (lax.broadcasted_iota(jnp.int32, (nb, slots), 0) == own_row[...]) & (
        lax.broadcasted_iota(jnp.int32, (nb, slots), 1) < count_s[0]
    )
    owner = jnp.where(own_mask, 1.0, 0.0).astype(BF16)
    owner3 = jnp.concatenate([owner, owner, owner], axis=1)

    for copy in aux_copies:
        copy.wait()
    take_row = jnp.full((8, BLK), arow_s[0, 0].astype(F32)) > 0.5
    take_col = jnp.full((8, BLK), acol_s[0, 0].astype(F32)) > 0.5
    take_far = jnp.broadcast_to(got_aux[1, 2:3, :], (8, BLK)) > 0.5

    def chosen(mine, by_row, by_col, by_both):
        far = jnp.where(take_far, by_both, by_col)
        close = jnp.where(take_row, by_row, mine)
        return jnp.where(take_col, far, close)

    centre = chosen(aux[...], got_aux[0], got_aux[1], got_aux[2])
    centres = [centre[0:1, :], centre[1:2, :]]

    def take_window(source, got):
        for c in range(3):
            for b in range(0, nb, 8):
                raw[c * nb + b : c * nb + b + 8, :] = chosen(
                    source[c, b : b + 8], got[0, c, b : b + 8], got[1, c, b : b + 8], got[2, c, b : b + 8]
                )

    for copy in x_copies:
        copy.wait()
    take_window(pos, got_x)

    def store_x(k, b, line):
        xs[k, pl.ds(b, 1), :] = line

    def store_v(k, b, line):
        vs[k, pl.ds(b, 1), :] = line

    permuted(raw[...], 3, store_x)

    def take_velocities():
        for copy in v_copies:
            copy.wait()
        take_window(vel, got_v)
        permuted(raw[...], 3, store_v)

    def force(e, meanwhile):
        near = nears[e]
        x = xs[...]
        near[1] = x * SCALE
        up = pltpu.make_async_remote_copy(
            src_ref=near.at[1],
            dst_ref=near.at[0],
            send_sem=halo_send.at[e, 0],
            recv_sem=halo_recv.at[e, 0],
            device_id=(row, col, lax.rem(me + 1, doms)),
            device_id_type=MESH,
        )
        down = pltpu.make_async_remote_copy(
            src_ref=near.at[1],
            dst_ref=near.at[2],
            send_sem=halo_send.at[e, 1],
            recv_sem=halo_recv.at[e, 1],
            device_id=(row, col, lax.rem(me + doms - 1, doms)),
            device_id_type=MESH,
        )

        @pl.when(me < doms - 1)
        def _():
            up.start()

        @pl.when(me > 0)
        def _():
            down.start()

        for k in range(2):
            part = jnp.sum(ws[k] * x, axis=0)
            parts[e, me, k] = jnp.sum(part.reshape(nb // 8, 8, BLK), axis=0)
        part_copies = []
        for at, target in enumerate(others):
            copy = pltpu.make_async_remote_copy(
                src_ref=parts.at[e, me],
                dst_ref=parts.at[e, me],
                send_sem=part_send.at[e, at],
                recv_sem=part_recv.at[e, at],
                device_id=target,
                device_id_type=MESH,
            )
            copy.start()
            part_copies.append(copy)

        meanwhile()

        @pl.when(me < doms - 1)
        def _():
            up.wait_send()
            down.wait_recv()

        @pl.when(me > 0)
        def _():
            down.wait_send()
            up.wait_recv()

        unroll = 2

        def slot(p):
            own = own_s[0, p]
            other = other_s[0, p]
            slab = lax.div(other, nb)
            block = lax.rem(other, nb)
            mine = [jnp.broadcast_to(near[1, k, pl.ds(own, 1), :], (8, BLK)) for k in range(3)]
            theirs = [jnp.broadcast_to(near[slab, k, pl.ds(block, 1), :], (8, BLK)) for k in range(3)]
            tile = jnp.where(lines == 0, theirs[0], jnp.where(lines == 1, theirs[1], theirs[2]))
            turned = jnp.transpose(tile)
            total = [None, None, None]
            for j in range(BLK // 8):
                at = slice(8 * j, 8 * j + 8)
                apart = [mine[k] - jnp.broadcast_to(turned[at, k : k + 1], (8, BLK)) for k in range(3)]
                squared = apart[0] * apart[0] + apart[1] * apart[1] + apart[2] * apart[2]
                weight = jnp.exp2(-squared)
                for k in range(3):
                    term = weight * apart[k]
                    total[k] = term if j == 0 else total[k] + term
            for k in range(3):
                tiles[k, pl.ds(p, 1), :] = jnp.sum(total[k], axis=0, keepdims=True)

        def body(i, carry):
            for u in range(unroll):
                slot(i * unroll + u)
            return carry

        lax.fori_loop(0, slots // unroll, body, 0)

        for copy in part_copies:
            copy.wait()
        sums = parts[e, 0]
        for d in range(1, doms):
            sums = sums + parts[e, d]
        pulls = []
        for k in range(2):
            collective = jnp.sum(sums[k], axis=(0, 1), keepdims=True)
            pulls.append(stiff_s[k] * (collective - centres[k]))
        for k in range(3):
            pair = jnp.dot(owner3, stacked_split(tiles[k]), preferred_element_type=F32)
            fs[k] = (PAIR_EPS / SCALE) * pair - pulls[0] * ws[0, k] - pulls[1] * ws[1, k]

    force(0, take_velocities)
    for step in range(STEPS):
        half = 0.5 * DT * ms[...]
        for k in range(3):
            v = vs[k] + half * fs[k]
            vs[k] = v
            xs[k] = xs[k] + DT * v
        if step < STEPS - 1:
            force(step + 1, lambda: None)
            for k in range(3):
                vs[k] = vs[k] + half * fs[k]

    def write_positions():
        out_x[...] = unpermuted(xs)
        out_v[...] = unpermuted(vs)

    force(STEPS, write_positions)
    forces = unpermuted(fs)
    out_f[...] = forces
    out_v[...] = out_v[...] + (0.5 * DT) * mass[...][None] * forces


def per_device(
    positions, velocities, inv_mass, cv_weight, stiffness, centers, block_order, pair_count, pair_own, pair_other,
    accept_row, accept_col,
):
    atoms = block_order.shape[0]
    nb = atoms // BLK
    slots = pair_own.shape[1]
    doms = lax.axis_size("dom")
    evals = STEPS + 1
    vmem = pl.BlockSpec(memory_space=pltpu.VMEM)
    smem = pl.BlockSpec(memory_space=pltpu.SMEM)
    dma = pltpu.SemaphoreType.DMA
    shape = jax.ShapeDtypeStruct((3, nb, BLK), F32)
    outs = pl.pallas_call(
        functools.partial(kernel, (doms, nb, slots)),
        out_shape=(shape, shape, shape),
        in_specs=[vmem] * 6 + [smem] * 7,
        out_specs=(vmem, vmem, vmem),
        scratch_shapes=[
            pltpu.VMEM((BLK, atoms), BF16),
            pltpu.VMEM((nb, BLK), jnp.int32),
            pltpu.VMEM((3 * nb, BLK), F32),
            pltpu.VMEM((7 * nb, BLK), F32),
            pltpu.VMEM((3, 3, nb, BLK), F32),
            pltpu.VMEM((3, 3, nb, BLK), F32),
            pltpu.VMEM((3, 8, BLK), F32),
            pltpu.VMEM((8, BLK), F32),
            pltpu.VMEM((evals, doms, 2, 8, BLK), F32),
            pltpu.VMEM((3, slots, BLK), F32),
            pltpu.VMEM((3, nb, BLK), F32),
            pltpu.VMEM((3, nb, BLK), F32),
            pltpu.VMEM((3, nb, BLK), F32),
            pltpu.VMEM((nb, BLK), F32),
            pltpu.VMEM((2, 3, nb, BLK), F32),
            dma((3,)), dma((3,)), dma((3,)), dma((3,)), dma((3,)), dma((3,)),
            dma((evals, 2)), dma((evals, 2)), dma((evals, doms)), dma((evals, doms)),
        ]
        + [pltpu.VMEM((3, 3, nb, BLK), F32)] * evals,
        compiler_params=pltpu.CompilerParams(collective_id=0, has_side_effects=True),
        name="windows",
    )(
        positions.reshape(3, nb, BLK), velocities.reshape(3, nb, BLK), inv_mass.reshape(nb, BLK), cv_weight, block_order.reshape(nb, BLK), pair_own,
        pair_own, pair_other, pair_count, stiffness, centers[0], accept_row, accept_col,
    )
    return tuple(out.reshape(1, 1, 3, atoms) for out in outs)


def solution(mesh):
    placed = (
        P("wrow", "wcol", None, "dom"),
        P("wrow", "wcol", None, "dom"),
        P("dom"),
        P(None, None, "dom"),
        P(),
        P("wrow", "wcol", None),
        P("dom"),
        P("dom"),
        P("dom", None),
        P("dom", None),
        P("wrow", "wcol"),
        P("wrow", "wcol"),
    )
    return jax.shard_map(
        per_device,
        mesh=mesh,
        in_specs=placed,
        out_specs=(
            P("wrow", "wcol", None, "dom"),
            P("wrow", "wcol", None, "dom"),
            P("wrow", "wcol", None, "dom"),
        ),
        check_vma=False,
    )
```

```python
import functools
import math

import numpy as np
import jax
import jax.numpy as jnp
from jax import lax
from jax.experimental import pallas as pl
from jax.experimental.pallas import tpu as pltpu
from jax.sharding import PartitionSpec as P

BLK = 128
STEPS = 3
PAIR_EPS = 0.015625
DT = 0.1
SCALE = math.sqrt(math.log2(math.e))
ROWS = 32
UNROLL = 8
OTHER_ROWS = {0: 0, 1: 1, 2: 2, 3: 3, 4: 4, 5: 5, 6: 9, 7: 9, 8: 9, 9: 6, 10: 7, 11: 8, 16: 0, 17: 1, 18: 2, 19: 3, 20: 4, 21: 5}
OWN_ROWS = {0: 0, 1: 1, 2: 2, 3: 0, 4: 1, 5: 2, 6: 6, 7: 7, 8: 8, 9: 9, 10: 9, 11: 9, 16: 3, 17: 4, 18: 5, 19: 3, 20: 4, 21: 5}
MESH = pl.DeviceIdType.MESH
F32 = jnp.float32
BF16 = jnp.bfloat16


def split3(value):
    high = value.astype(BF16)
    rest = value - high.astype(F32)
    middle = rest.astype(BF16)
    low = (rest - middle.astype(F32)).astype(BF16)
    return high, middle, low


def stacked_split(value):
    return jnp.concatenate(split3(value), axis=0)


def unsplit(value, rows):
    return value[0:rows] + (value[rows : 2 * rows] + value[2 * rows : 3 * rows])


def placing(rows_of, nb):
    table = np.zeros((nb, ROWS, 10, nb), np.float32)
    for row, kind in rows_of.items():
        for b in range(nb):
            table[b, row, kind, b] = 1.0
    return jnp.asarray(table.reshape(nb * ROWS, 10 * nb), BF16)


def kernel(
    sizes,
    pos, vel, mass, cvw, order, own_row, place_own, place_other, own_s, other_s, count_s, stiff_s, centers_s, arow_s, acol_s,
    out_x, out_v, out_f,
    onehot, high_block, raw, raw_w, got_x, got_v, got_aux, aux, parts, tiles, others_of, turned_own, summing, xs, vs, fs, ms, ws,
    sx_send, sx_recv, sv_send, sv_recv, sa_send, sa_recv, halo_send, halo_recv, part_send, part_recv, *nears,
):
    doms, nb, slots = sizes
    row = lax.axis_index("wrow")
    col = lax.axis_index("wcol")
    me = lax.axis_index("dom")
    row_to = row + 1 - 2 * lax.rem(row, 2)
    col_to = col + 1 - 2 * lax.rem(col, 2)
    partners = [(row_to, col, me), (row, col_to, me), (row_to, col_to, me)]
    others = [(row, col, lax.rem(me + off, doms)) for off in range(1, doms)]

    lines = lax.broadcasted_iota(jnp.int32, (8, BLK), 0)
    aux[...] = jnp.where(
        lines == 0,
        centers_s[0, 0],
        jnp.where(lines == 1, centers_s[0, 1], arow_s[0, 0].astype(F32)),
    )
    for held in nears:
        held[...] = jnp.zeros(held.shape, F32)
    barrier = pltpu.get_barrier_semaphore()
    for target in partners + others:
        pl.semaphore_signal(barrier, inc=1, device_id=target, device_id_type=MESH)
    pl.semaphore_wait(barrier, len(partners) + len(others))

    def exchange(source, target, sends, recvs):
        copies = []
        for at, partner in enumerate(partners):
            copy = pltpu.make_async_remote_copy(
                src_ref=source,
                dst_ref=target.at[at],
                send_sem=sends.at[at],
                recv_sem=recvs.at[at],
                device_id=partner,
                device_id_type=MESH,
            )
            copy.start()
            copies.append(copy)
        return copies

    aux_copies = exchange(aux, got_aux, sa_send, sa_recv)
    x_copies = exchange(pos, got_x, sx_send, sx_recv)
    v_copies = exchange(vel, got_v, sv_send, sv_recv)

    jl = lax.broadcasted_iota(jnp.int32, (BLK, BLK), 0)
    listed = order[...]
    low = lax.rem(listed, BLK)
    high_block[...] = lax.div(listed, BLK)
    for b in range(nb):
        onehot[:, b * BLK : (b + 1) * BLK] = jnp.where(low[b : b + 1, :] == jl, 1.0, 0.0).astype(BF16)
    jb_lines = lax.broadcasted_iota(jnp.int32, (nb, BLK), 0)

    def permuted(source, comps, store):
        split = stacked_split(source)

        def body(b, carry):
            at = pl.ds(pl.multiple_of(b * BLK, BLK), BLK)
            picked = jnp.dot(split, onehot[:, at], preferred_element_type=F32)
            picked = unsplit(picked, comps * nb)
            mask = high_block[pl.ds(b, 1), :] == jb_lines
            for k in range(comps):
                line = jnp.sum(jnp.where(mask, picked[k * nb : (k + 1) * nb], 0.0), axis=0, keepdims=True)
                store(k, b, line)
            return carry

        lax.fori_loop(0, nb, body, 0, unroll=True)

    def unpermuted(source_ref):
        def body(b, total):
            at = pl.ds(pl.multiple_of(b * BLK, BLK), BLK)
            mask = high_block[pl.ds(b, 1), :] == jb_lines
            spread = jnp.concatenate(
                [jnp.where(mask, source_ref[k, pl.ds(b, 1), :], 0.0) for k in range(3)], axis=0
            )
            return total + lax.dot_general(
                stacked_split(spread), onehot[:, at], (((1,), (1,)), ((), ())), preferred_element_type=F32
            )

        total = lax.fori_loop(0, nb, body, jnp.zeros((9 * nb, BLK), F32), unroll=True)
        return unsplit(total, 3 * nb).reshape(3, nb, BLK)

    for b in range(nb):
        at = slice(b * BLK, (b + 1) * BLK)
        for k in range(2):
            for c in range(3):
                raw_w[(3 * k + c) * nb + b : (3 * k + c) * nb + b + 1, :] = cvw[k, c : c + 1, at]
    raw_w[6 * nb : 7 * nb, :] = mass[...]

    def store_w(k, b, line):
        if k < 6:
            ws[k // 3, k % 3, pl.ds(b, 1), :] = line
        else:
            ms[pl.ds(b, 1), :] = line

    permuted(raw_w[...], 7, store_w)

    wide = 8 * slots
    at_slot = lax.div(lax.broadcasted_iota(jnp.int32, (slots, wide), 1), 8)
    spread_slots = jnp.where(at_slot == lax.broadcasted_iota(jnp.int32, (slots, wide), 0), 1.0, 0.0).astype(BF16)
    live = lax.broadcasted_iota(jnp.int32, (8, slots), 1) < count_s[0]
    owners = jnp.where(live, jnp.broadcast_to(own_row[...], (8, slots)).astype(F32), -1.0).astype(BF16)
    owners = jnp.dot(owners, spread_slots, preferred_element_type=F32)[0:1, :]
    block_line = lax.broadcasted_iota(jnp.int32, (nb, wide), 0).astype(F32)
    row_line = lax.rem(lax.broadcasted_iota(jnp.int32, (nb, wide), 1), 8)
    for r in range(7):
        summing[r * nb : (r + 1) * nb, :] = jnp.where(
            (owners == block_line) & (row_line == r), 1.0, 0.0
        ).astype(BF16)

    for copy in aux_copies:
        copy.wait()
    take_row = jnp.full((8, BLK), arow_s[0, 0].astype(F32)) > 0.5
    take_col = jnp.full((8, BLK), acol_s[0, 0].astype(F32)) > 0.5
    take_far = jnp.broadcast_to(got_aux[1, 2:3, :], (8, BLK)) > 0.5

    def chosen(mine, by_row, by_col, by_both):
        far = jnp.where(take_far, by_both, by_col)
        close = jnp.where(take_row, by_row, mine)
        return jnp.where(take_col, far, close)

    centre = chosen(aux[...], got_aux[0], got_aux[1], got_aux[2])
    centres = [centre[0:1, :], centre[1:2, :]]

    def take_window(source, got):
        for c in range(3):
            for b in range(0, nb, 8):
                raw[c * nb + b : c * nb + b + 8, :] = chosen(
                    source[c, b : b + 8], got[0, c, b : b + 8], got[1, c, b : b + 8], got[2, c, b : b + 8]
                )

    for copy in x_copies:
        copy.wait()
    take_window(pos, got_x)

    def store_x(k, b, line):
        xs[k, pl.ds(b, 1), :] = line

    def store_v(k, b, line):
        vs[k, pl.ds(b, 1), :] = line

    permuted(raw[...], 3, store_x)

    def take_velocities():
        for copy in v_copies:
            copy.wait()
        take_window(vel, got_v)
        permuted(raw[...], 3, store_v)

    def force(e, meanwhile):
        near = nears[e]
        x = xs[...]
        near[1] = x * SCALE
        up = pltpu.make_async_remote_copy(
            src_ref=near.at[1],
            dst_ref=near.at[0],
            send_sem=halo_send.at[e, 0],
            recv_sem=halo_recv.at[e, 0],
            device_id=(row, col, lax.rem(me + 1, doms)),
            device_id_type=MESH,
        )
        down = pltpu.make_async_remote_copy(
            src_ref=near.at[1],
            dst_ref=near.at[2],
            send_sem=halo_send.at[e, 1],
            recv_sem=halo_recv.at[e, 1],
            device_id=(row, col, lax.rem(me + doms - 1, doms)),
            device_id_type=MESH,
        )

        @pl.when(me < doms - 1)
        def _():
            up.start()

        @pl.when(me > 0)
        def _():
            down.start()

        for k in range(2):
            part = jnp.sum(ws[k] * x, axis=0)
            parts[e, me, k] = jnp.sum(part.reshape(nb // 8, 8, BLK), axis=0)
        part_copies = []
        for at, target in enumerate(others):
            copy = pltpu.make_async_remote_copy(
                src_ref=parts.at[e, me],
                dst_ref=parts.at[e, me],
                send_sem=part_send.at[e, at],
                recv_sem=part_recv.at[e, at],
                device_id=target,
                device_id_type=MESH,
            )
            copy.start()
            part_copies.append(copy)

        def features(slab):
            highs, middles, held = [], [], []
            for k in range(3):
                value = near[slab, k]
                high = value.astype(BF16)
                middle = (value - high.astype(F32)).astype(BF16)
                highs.append(high)
                middles.append(middle)
                held.append(high.astype(F32) + middle.astype(F32))
            norm = -0.5 * (held[0] * held[0] + held[1] * held[1] + held[2] * held[2])
            ones = jnp.ones((nb, BLK), BF16)
            return jnp.concatenate(highs + middles + list(split3(norm)) + [ones], axis=0), held

        def place_others(slab, kinds):
            placed = jnp.dot(place_other[...], kinds, preferred_element_type=F32).astype(BF16)
            others_of[slab * nb : (slab + 1) * nb] = placed.reshape(nb, ROWS, BLK)

        kinds, held = features(1)
        place_others(1, kinds)
        placed = jnp.dot(place_own[...], kinds, preferred_element_type=F32)
        for b in range(nb):
            turned_own[b] = jnp.transpose(placed[b * ROWS : (b + 1) * ROWS]).astype(BF16)

        meanwhile()

        @pl.when(me < doms - 1)
        def _():
            up.wait_send()
            down.wait_recv()

        @pl.when(me > 0)
        def _():
            down.wait_send()
            up.wait_recv()

        place_others(0, features(0)[0])
        place_others(2, features(2)[0])

        def slots_at(first):
            for p in [first + u for u in range(UNROLL)]:
                theirs = others_of[other_s[0, p]]
                weight = jnp.exp2(jnp.dot(turned_own[own_s[0, p]], theirs, preferred_element_type=F32))
                high = weight.astype(BF16)
                low = (weight - high.astype(F32)).astype(BF16)
                lines_of = theirs[0:16, :]
                pulled = lax.dot_general(
                    jnp.concatenate([lines_of, lines_of], axis=1),
                    jnp.concatenate([high, low], axis=1),
                    (((1,), (1,)), ((), ())),
                    preferred_element_type=F32,
                )
                tiles[p] = pulled[0:8, :]

        def body(i, carry):
            slots_at(i * UNROLL)
            return carry

        lax.fori_loop(0, slots // UNROLL, body, 0)

        for copy in part_copies:
            copy.wait()
        sums = parts[e, 0]
        for d in range(1, doms):
            sums = sums + parts[e, d]
        pulls = []
        for k in range(2):
            collective = jnp.sum(sums[k], axis=(0, 1), keepdims=True)
            pulls.append(stiff_s[k] * (collective - centres[k]))
        total = sum(
            jnp.dot(summing[...], term, preferred_element_type=F32)
            for term in split3(tiles[...].reshape(8 * slots, BLK))[::-1]
        )
        for k in range(3):
            pulled = total[k * nb : (k + 1) * nb] + total[(3 + k) * nb : (4 + k) * nb]
            pair = held[k] * total[6 * nb : 7 * nb] - pulled
            fs[k] = (PAIR_EPS / SCALE) * pair - pulls[0] * ws[0, k] - pulls[1] * ws[1, k]

    force(0, take_velocities)
    for step in range(STEPS):
        half = 0.5 * DT * ms[...]
        for k in range(3):
            v = vs[k] + half * fs[k]
            vs[k] = v
            xs[k] = xs[k] + DT * v
        if step < STEPS - 1:
            force(step + 1, lambda: None)
            for k in range(3):
                vs[k] = vs[k] + half * fs[k]

    def write_positions():
        out_x[...] = unpermuted(xs)
        out_v[...] = unpermuted(vs)

    force(STEPS, write_positions)
    forces = unpermuted(fs)
    out_f[...] = forces
    out_v[...] = out_v[...] + (0.5 * DT) * mass[...][None] * forces


def per_device(
    positions, velocities, inv_mass, cv_weight, stiffness, centers, block_order, pair_count, pair_own, pair_other,
    accept_row, accept_col,
):
    atoms = block_order.shape[0]
    nb = atoms // BLK
    slots = pair_own.shape[1]
    doms = lax.axis_size("dom")
    evals = STEPS + 1
    vmem = pl.BlockSpec(memory_space=pltpu.VMEM)
    smem = pl.BlockSpec(memory_space=pltpu.SMEM)
    dma = pltpu.SemaphoreType.DMA
    shape = jax.ShapeDtypeStruct((3, nb, BLK), F32)
    outs = pl.pallas_call(
        functools.partial(kernel, (doms, nb, slots)),
        out_shape=(shape, shape, shape),
        in_specs=[vmem] * 8 + [smem] * 7,
        out_specs=(vmem, vmem, vmem),
        scratch_shapes=[
            pltpu.VMEM((BLK, atoms), BF16),
            pltpu.VMEM((nb, BLK), jnp.int32),
            pltpu.VMEM((3 * nb, BLK), F32),
            pltpu.VMEM((7 * nb, BLK), F32),
            pltpu.VMEM((3, 3, nb, BLK), F32),
            pltpu.VMEM((3, 3, nb, BLK), F32),
            pltpu.VMEM((3, 8, BLK), F32),
            pltpu.VMEM((8, BLK), F32),
            pltpu.VMEM((evals, doms, 2, 8, BLK), F32),
            pltpu.VMEM((slots, 8, BLK), F32),
            pltpu.VMEM((3 * nb, ROWS, BLK), BF16),
            pltpu.VMEM((nb, BLK, ROWS), BF16),
            pltpu.VMEM((7 * nb, 8 * slots), BF16),
            pltpu.VMEM((3, nb, BLK), F32),
            pltpu.VMEM((3, nb, BLK), F32),
            pltpu.VMEM((3, nb, BLK), F32),
            pltpu.VMEM((nb, BLK), F32),
            pltpu.VMEM((2, 3, nb, BLK), F32),
            dma((3,)), dma((3,)), dma((3,)), dma((3,)), dma((3,)), dma((3,)),
            dma((evals, 2)), dma((evals, 2)), dma((evals, doms)), dma((evals, doms)),
        ]
        + [pltpu.VMEM((3, 3, nb, BLK), F32)] * evals,
        compiler_params=pltpu.CompilerParams(collective_id=0, has_side_effects=True),
        name="windows",
    )(
        positions.reshape(3, nb, BLK), velocities.reshape(3, nb, BLK), inv_mass.reshape(nb, BLK), cv_weight, block_order.reshape(nb, BLK), pair_own,
        placing(OWN_ROWS, nb), placing(OTHER_ROWS, nb), pair_own, pair_other, pair_count, stiffness, centers[0], accept_row, accept_col,
    )
    return tuple(out.reshape(1, 1, 3, atoms) for out in outs)


def solution(mesh):
    placed = (
        P("wrow", "wcol", None, "dom"),
        P("wrow", "wcol", None, "dom"),
        P("dom"),
        P(None, None, "dom"),
        P(),
        P("wrow", "wcol", None),
        P("dom"),
        P("dom"),
        P("dom", None),
        P("dom", None),
        P("wrow", "wcol"),
        P("wrow", "wcol"),
    )
    return jax.shard_map(
        per_device,
        mesh=mesh,
        in_specs=placed,
        out_specs=(
            P("wrow", "wcol", None, "dom"),
            P("wrow", "wcol", None, "dom"),
            P("wrow", "wcol", None, "dom"),
        ),
        check_vma=False,
    )
```
